32 devices in a mesh: lat: 8 (over z, x), lon: 4 (over y, core).
Axes of the slice: x: 2, y: 2, z: 4, core: 2. Of those that a mesh axis runs over, the one named last changes fastest.
Arguments:
- increment: bfloat16 [16, 8, 144, 128], P('lat', 'lon'), may hold values from -6 to 6
- cotangent: bfloat16 [8, 4, 40, 144, 128], P('lat', 'lon'), may hold values from -6 to 6
- weights: bfloat16 [8, 4, 40, 16, 128, 128], P('lat', 'lon'), may hold values from -0.1875 to 0.1875
- source_ids: int32 [8, 4, 40, 16], P('lat', 'lon'), may hold values from 0 to 127, as said below
- counts: int32 [8, 4, 40], P('lat', 'lon'), may hold values from 0 to 16, as said below
Outputs:
- ocean: bfloat16 [8, 4, 40, 144, 128], P('lat', 'lon')
- atmos_adjoint: bfloat16 [16, 8, 144, 128], P('lat', 'lon')
The draws below stay inside these ranges and needn't reach their ends.
Inputs may be any that keep to these rules, and one draw needn't show every extreme that they name: source_ids[i, j, t, k] = a * 8 + b with block row a between i * 2 - 1 and (i + 1) * 2, and block column b equal, modulo 8, to one of j * 2 - 1 to (j + 1) * 2. `counts`: every device's tile (i, j) has some target block with exactly 16 live slots.
All inputs are finite; a program needn't handle non-finite values.
Results may differ from the reference program's by a relative error of at most 0.001.
Values may be sent and summed in bfloat16 or wider, within the bound.
A program may use at most 192 MiB of HBM per device.

```python
import jax
import jax.numpy as jnp
from jax import lax

BS = 128
BT = 128
SBD = 2
TB = 40
KPT = 16
ROWS = 144
NLB = 16
NOB = 8
N_LAT = 8
N_LON = 4


def draw_source_ids(key, part):
    key_rows, key_cols = jax.random.split(jax.random.fold_in(key, 11))
    shape = (N_LAT, N_LON, TB, KPT)
    lat_grid = jnp.arange(N_LAT, dtype=jnp.int32)[:, None, None, None]
    lon_grid = jnp.arange(N_LON, dtype=jnp.int32)[None, :, None, None]
    lowest = jnp.where(lat_grid == 0, 1, 0)
    highest = jnp.where(lat_grid == N_LAT - 1, SBD, SBD + 1)
    raw_rows = jax.random.randint(key_rows, shape, 0, 1 << 20)
    ext_row = lowest + raw_rows % (highest - lowest + 1)
    ext_col = jax.random.randint(key_cols, shape, 0, SBD + 2)
    cycle_blocks = SBD * N_LON
    block_row = lat_grid * SBD + ext_row - 1
    block_col = (lon_grid * SBD + ext_col - 1 + cycle_blocks) % cycle_blocks
    return (block_row * cycle_blocks + block_col).astype(jnp.int32)


def draw_counts(key, part):
    key_rows, key_cols = jax.random.split(jax.random.fold_in(key, 23))
    drawn = jax.random.randint(key_rows, (N_LAT, N_LON, TB), 0, KPT + 1)
    full_slot = jax.random.randint(key_cols, (N_LAT, N_LON, 1), 0, TB)
    target_index = jnp.arange(TB, dtype=jnp.int32)[None, None, :]
    return jnp.where(target_index == full_slot, KPT, drawn).astype(jnp.int32)


def block_levels(key, extent, cuts, low, largest):
    factor_of = 1.0
    for dim, blocks in cuts:
        steps = jax.random.uniform(jax.random.fold_in(jax.random.fold_in(key, 6), dim), (blocks,), jnp.float32, low / len(cuts), largest / len(cuts))
        factor_of = factor_of * jnp.repeat(jnp.exp(steps), extent[dim] // blocks).reshape((-1,) + (1,) * (len(extent) - 1 - dim))
    return factor_of


def scatter_about(key, extent, width, limit, cuts=(), kind=jnp.bfloat16):
    gain = block_levels(key, extent, cuts, -0.22, 0.18) if cuts else 1.0
    entries = jax.random.normal(key, extent, jnp.float32) * width * gain
    return jnp.minimum(jnp.maximum(entries, -limit), limit).astype(kind)


def setup_inputs(seed: int = 0) -> dict:
    streams_of = jax.random.split(jax.random.key(seed), 6)
    return {
        "increment": scatter_about(streams_of[0], (NLB, NOB, ROWS, BS), 1.0, 6.0, ((0, 8), (1, 4))),
        "cotangent": scatter_about(streams_of[1], (N_LAT, N_LON, TB, ROWS, BT), 1.0, 6.0, ((0, 8), (1, 4))),
        "weights": scatter_about(streams_of[2], (N_LAT, N_LON, TB, KPT, BS, BT), (BS * KPT // 2) ** -0.5, 0.1875, ((0, 8), (1, 4))),
        "source_ids": draw_source_ids(jax.random.fold_in(streams_of[5], 71), 0),
        "counts": draw_counts(jax.random.fold_in(streams_of[5], 71), 0),
    }


def reference(increment, cotangent, weights, source_ids, counts):
    total_blocks = NLB * NOB
    device_count = N_LAT * N_LON
    flattened = increment.reshape(total_blocks, ROWS, BS)
    weight_all = weights.reshape(device_count, TB, KPT, BS, BT)
    source_all = source_ids.reshape(device_count, TB, KPT).astype(jnp.int32)
    count_all = counts.reshape(device_count, TB).astype(jnp.int32)
    cotan_all = cotangent.reshape(device_count, TB, ROWS, BT)

    def device_step(running, pieces):
        weight_dev, source_dev, count_dev, cotan_dev = pieces
        ocean_sum = jnp.zeros((TB, ROWS, BT), jnp.float32)
        cotan_wide = cotan_dev.astype(jnp.float32)
        for slot in range(KPT):
            active = slot < count_dev
            weight_slot = weight_dev[:, slot].astype(jnp.float32)
            picked = flattened[source_dev[:, slot]].astype(jnp.float32) * active.astype(jnp.float32)[:, None, None]
            ocean_sum = ocean_sum + jnp.einsum("tws,tsb->twb", picked, weight_slot)
            contribution = jnp.einsum("twb,tsb->tws", cotan_wide, weight_slot)
            segment = jnp.where(active, source_dev[:, slot], total_blocks).astype(jnp.int32)
            running = running.at[segment].add(contribution)
        return running, ocean_sum.astype(jnp.bfloat16)

    running = jnp.zeros((total_blocks + 1, ROWS, BS), jnp.float32)
    running, ocean = lax.scan(device_step, running, (weight_all, source_all, count_all, cotan_all))
    ocean = ocean.reshape(N_LAT, N_LON, TB, ROWS, BT)
    adjoint_out = running[:total_blocks].reshape(NLB, NOB, ROWS, BS).astype(jnp.bfloat16)
    return ocean, adjoint_out
```

```python
import functools

import jax
import jax.numpy as jnp
from jax import lax
from jax.experimental import pallas as pl
from jax.experimental.pallas import tpu as pltpu
from jax.sharding import PartitionSpec as P

CHUNK = 16
UNROLL = 8
STEPS = 32767.0
WAYS = ((1, 1), (1, -1), (-1, 1), (-1, -1), (1, 0), (-1, 0), (0, 1), (0, -1))


def away(by, side):
    return [side + 1] if by > 0 else ([0] if by < 0 else list(range(1, side + 1)))


def edge_places(way, side):
    i, j = WAYS[way]
    return [r * (side + 2) + c for r in away(i, side) for c in away(j, side)]


def edge_start(way, side):
    return sum(len(edge_places(w, side)) for w in range(way))


def halo_copies(side):
    copies = []
    for way, (i, j) in enumerate(WAYS):
        sent = [side - 1] if i > 0 else ([0] if i < 0 else list(range(side)))
        held = away(-i, side)
        col = side - 1 if j > 0 else 0
        for r, h in zip(sent, held):
            copies.append((way, r, col, h * (side + 2) + away(-j, side)[0], 1 if j else side))
    return copies


def spread(side, lon_count, ids, counts):
    cycle = side * lon_count
    if cycle & (cycle - 1) == 0:
        row = lax.shift_right_logical(ids, cycle.bit_length() - 1)
        col = ids & (cycle - 1)
    else:
        row = lax.div(ids, cycle)
        col = ids - row * cycle
    ext_row = row - lax.axis_index("lat") * side + 1
    ext_col = col - lax.axis_index("lon") * side + 1
    ext_col = jnp.where(ext_col < 0, ext_col + cycle, ext_col)
    ext_col = jnp.where(ext_col >= cycle, ext_col - cycle, ext_col)
    width = side + 2
    slot = lax.broadcasted_iota(jnp.int32, ids.shape, 0)
    return jnp.where(slot < counts, ext_row * width + ext_col, width * width)


def adjoint_kernel(
    side, lon_count, ids_ref, counts_ref, cot_ref, w_ref, own_ref, code_ref, scale_ref, place_ref,
    acc, cot, w_vmem, ids, counts, live, place, of_target, of_slot, w_sems, sems,
):
    targets, slots = w_ref.shape[2:4]
    cells = w_ref.shape[4]
    width = side + 2
    trash = width * width
    live_copy = pltpu.make_async_copy(counts_ref.at[0], live, sems.at[0])
    counts_copy = pltpu.make_async_copy(counts_ref.at[0], counts, sems.at[1])
    ids_copy = pltpu.make_async_copy(ids_ref.at[0, 0], ids, sems.at[2])
    cot_copy = pltpu.make_async_copy(cot_ref.at[0, 0], cot, sems.at[3])
    live_copy.start()
    counts_copy.start()
    ids_copy.start()
    cot_copy.start()
    live_copy.wait()

    def pairs_of(t):
        return lax.shift_right_logical(live[0, t] + 1, 1)

    def weight_copy(t, at):
        n = pairs_of(t) * 2
        return pltpu.make_async_copy(
            w_ref.at[0, 0, t, pl.ds(0, n)], w_vmem.at[pl.ds(at * 2, n)], w_sems.at[t]
        )

    def issue(t, at):
        n = pairs_of(t)

        @pl.when(n > 0)
        def _():
            weight_copy(t, at).start()

        for j in range(slots // 2):
            of_target[at + j] = t
            of_slot[at + j] = 2 * j
        return at + n

    total = lax.fori_loop(0, targets, issue, 0)
    counts_copy.wait()
    ids_copy.wait()
    place_ref[...] = spread(side, lon_count, ids[...], counts[...])
    place_copy = pltpu.make_async_copy(place_ref, place, sems.at[4])
    place_copy.start()
    acc[...] = jnp.zeros_like(acc)
    cot_copy.wait()
    place_copy.wait()

    def chunk(c, met):
        base = c * CHUNK
        last = of_target[jnp.minimum(base + CHUNK, total) - 1]

        def meet(t, at):
            n = pairs_of(t)

            @pl.when(n > 0)
            def _():
                weight_copy(t, at).wait()

            return at

        lax.fori_loop(met, last + 1, meet, 0)
        for u in range(CHUNK):
            at = base + u
            there = at < total
            t = jnp.where(there, of_target[at], 0)
            k = jnp.where(there, of_slot[at], 0)
            both = lax.dot_general(
                cot[t],
                w_vmem[pl.ds(2 * at, 2)].reshape(2 * cells, cells),
                (((1,), (1,)), ((), ())),
                preferred_element_type=jnp.float32,
            )
            for m in range(2):
                to = jnp.where(there, place[k + m, t], trash)
                acc[to] += both[:, m * cells:(m + 1) * cells]
        return last + 1

    lax.fori_loop(0, lax.div(total + (CHUNK - 1), CHUNK), chunk, 0)
    for r in range(side):
        for c in range(side):
            own_ref[r, c] = acc[(r + 1) * width + c + 1]
    for way in range(len(WAYS)):
        for n, p in enumerate(edge_places(way, side)):
            block = acc[p]
            most = jnp.max(jnp.abs(block), axis=0, keepdims=True)
            steps = jnp.where(most > 0, STEPS / most, 0.0)
            at = edge_start(way, side) + n
            scale_ref[at] = most * (1.0 / STEPS)
            code_ref[at] = jnp.round(block * steps).astype(jnp.int32).astype(jnp.int16)


def exchange_kernel(
    sizes, place_ref, own_ref, part_ref, code_ref, scale_ref, w_ref, ocean_ref, out_ref,
    acc, ext, codes, scales, place, w_vmem, w_sems, sems, halo_send, halo_recv, code_send, code_recv,
    scale_send, scale_recv,
):
    lats, lons = sizes
    lat, lon = lax.axis_index("lat"), lax.axis_index("lon")
    side = out_ref.shape[0]
    width = side + 2
    targets, slots = w_vmem.shape[:2]
    cells = w_vmem.shape[2]
    barrier = pltpu.get_barrier_semaphore()

    def peer(i, j):
        return (lat + i, lax.rem(lon + j + lons, lons))

    def sends(i):
        return (lat + i >= 0) & (lat + i < lats)

    def gets(i):
        return (lat - i >= 0) & (lat - i < lats)

    for i, j in WAYS:
        @pl.when(sends(i))
        def _(i=i, j=j):
            pl.semaphore_signal(
                barrier, inc=1, device_id=peer(i, j), device_id_type=pl.DeviceIdType.MESH
            )

    def weights_of(t):
        return pltpu.make_async_copy(w_ref.at[0, 0, t], w_vmem.at[t], w_sems.at[t])

    place_copy = pltpu.make_async_copy(place_ref, place, sems.at[0])
    place_copy.start()

    @pl.loop(0, targets)
    def _(t):
        weights_of(t).start()

    halos = []
    for n, (way, row, col, to, wide) in enumerate(halo_copies(side)):
        halos.append((WAYS[way][0], pltpu.make_async_remote_copy(
            src_ref=own_ref.at[row, pl.ds(col, wide)],
            dst_ref=ext.at[pl.ds(to, wide)],
            send_sem=halo_send.at[n],
            recv_sem=halo_recv.at[n],
            device_id=peer(*WAYS[way]),
            device_id_type=pl.DeviceIdType.MESH,
        )))
    folds = []
    for way, (i, j) in enumerate(WAYS):
        span = pl.ds(edge_start(way, side), len(edge_places(way, side)))
        for from_ref, to_ref, send, recv in (
            (scale_ref, scales, scale_send, scale_recv), (code_ref, codes, code_send, code_recv)
        ):
            folds.append((i, pltpu.make_async_remote_copy(
                src_ref=from_ref.at[span],
                dst_ref=to_ref.at[span],
                send_sem=send.at[way],
                recv_sem=recv.at[way],
                device_id=peer(i, j),
                device_id_type=pl.DeviceIdType.MESH,
            )))
    north = (lat > 0).astype(jnp.int32)
    south = (lat < lats - 1).astype(jnp.int32)
    pl.semaphore_wait(barrier, 2 + 3 * north + 3 * south)
    for i, copy in halos + folds:
        pl.when(sends(i))(copy.start)
    acc[...] = part_ref[...]
    for r in range(side):
        for c in range(side):
            ext[(r + 1) * width + c + 1] = own_ref[r, c]
    blank = jnp.zeros(ext.shape[1:], ext.dtype)
    ext[width * width] = blank
    for i, row in ((1, 0), (-1, side + 1)):
        @pl.when(jnp.logical_not(gets(i)))
        def _(row=row):
            for c in range(width):
                ext[row * width + c] = blank
    place_copy.wait()
    for i, copy in halos:
        pl.when(gets(i))(copy.wait_recv)

    @pl.loop(0, targets // UNROLL)
    def _(g):
        for u in range(UNROLL):
            weights_of(g * UNROLL + u).wait()
        for u in range(UNROLL):
            t = g * UNROLL + u
            picked = jnp.concatenate([ext[place[k, t]] for k in range(slots)], axis=1)
            blocks = w_vmem[t].reshape(slots * cells, w_vmem.shape[3])
            total = jnp.dot(picked, blocks, preferred_element_type=jnp.float32)
            ocean_ref[0, 0, t] = total.astype(ocean_ref.dtype)

    for i, copy in folds:
        pl.when(gets(i))(copy.wait_recv)
    for way, (i, j) in enumerate(WAYS):
        rows = [r - 1 for r in away(-i, side)] if i == 0 else [0 if i > 0 else side - 1]
        cols = [c - 1 for c in away(-j, side)] if j == 0 else [0 if j > 0 else side - 1]

        @pl.when(gets(i))
        def _(way=way, rows=rows, cols=cols):
            for n, (r, c) in enumerate((r, c) for r in rows for c in cols):
                at = edge_start(way, side) + n
                acc[r, c] += codes[at].astype(jnp.int32).astype(jnp.float32) * scales[at]

    out_ref[...] = acc[...].astype(out_ref.dtype)
    for i, copy in halos + folds:
        pl.when(sends(i))(copy.wait_send)


def body(increment, cotangent, weights, source_ids, counts):
    side, _, levels, cells = increment.shape
    sizes = lax.axis_size("lat"), lax.axis_size("lon")
    vmem = pl.BlockSpec(memory_space=pltpu.VMEM)
    hbm = pl.BlockSpec(memory_space=pltpu.HBM)
    targets, slots = weights.shape[2:4]
    width = side + 2
    flat = (width * width + 1, levels, cells)
    edges = edge_start(len(WAYS), side)
    hops = len(halo_copies(side))
    pairs = targets * slots // 2
    cost = pl.CostEstimate(
        flops=2 * targets * slots * levels * cells * cells,
        bytes_accessed=weights.size * 2,
        transcendentals=0,
    )
    limit = 50 * 1024 * 1024
    own, code, scale, place = pl.pallas_call(
        functools.partial(adjoint_kernel, side, sizes[1]),
        out_shape=[
            jax.ShapeDtypeStruct(increment.shape, jnp.float32),
            jax.ShapeDtypeStruct((edges, levels, cells), jnp.int16),
            jax.ShapeDtypeStruct((edges, 1, cells), jnp.float32),
            jax.ShapeDtypeStruct((slots, targets), jnp.int32),
        ],
        in_specs=[hbm, hbm, hbm, hbm],
        out_specs=[vmem, vmem, vmem, vmem],
        scratch_shapes=[
            pltpu.VMEM(flat, jnp.float32),
            pltpu.VMEM(cotangent.shape[2:], cotangent.dtype),
            pltpu.VMEM((targets * slots + 2 * CHUNK, cells, weights.shape[5]), weights.dtype),
            pltpu.VMEM((slots, targets), jnp.int32),
            pltpu.VMEM((1, targets), jnp.int32),
            pltpu.SMEM((1, targets), jnp.int32),
            pltpu.SMEM((slots, targets), jnp.int32),
            pltpu.SMEM((pairs + CHUNK + slots,), jnp.int32),
            pltpu.SMEM((pairs + CHUNK + slots,), jnp.int32),
            pltpu.SemaphoreType.DMA((targets,)),
            pltpu.SemaphoreType.DMA((5,)),
        ],
        compiler_params=pltpu.CompilerParams(vmem_limit_bytes=limit),
        cost_estimate=cost,
        name="adjoint",
    )(jnp.swapaxes(source_ids, 2, 3), counts, cotangent, weights)
    ways = len(WAYS)
    return pl.pallas_call(
        functools.partial(exchange_kernel, sizes),
        out_shape=[
            jax.ShapeDtypeStruct(cotangent.shape, jnp.bfloat16),
            jax.ShapeDtypeStruct(increment.shape, jnp.bfloat16),
        ],
        in_specs=[vmem, vmem, vmem, vmem, vmem, hbm],
        out_specs=[vmem, vmem],
        scratch_shapes=[
            pltpu.VMEM(increment.shape, jnp.float32),
            pltpu.VMEM(flat, increment.dtype),
            pltpu.VMEM((edges, levels, cells), jnp.int16),
            pltpu.VMEM((edges, 1, cells), jnp.float32),
            pltpu.SMEM((slots, targets), jnp.int32),
            pltpu.VMEM(weights.shape[2:], weights.dtype),
            pltpu.SemaphoreType.DMA((targets,)),
            pltpu.SemaphoreType.DMA((1,)),
        ] + [pltpu.SemaphoreType.DMA((hops,))] * 2 + [pltpu.SemaphoreType.DMA((ways,))] * 4,
        compiler_params=pltpu.CompilerParams(
            collective_id=0, has_side_effects=True, vmem_limit_bytes=limit
        ),
        cost_estimate=cost,
        name="exchange",
    )(place, increment, own, code, scale, weights)


def solution(mesh):
    placed = (
        P("lat", "lon", None, None),
        P("lat", "lon", None, None, None),
        P("lat", "lon", None, None, None, None),
        P("lat", "lon", None, None),
        P("lat", "lon", None),
    )
    return jax.shard_map(
        body,
        mesh=mesh,
        in_specs=placed,
        out_specs=(P("lat", "lon", None, None, None), P("lat", "lon", None, None)),
        check_vma=False,
    )
```

```python
import functools

import jax
import jax.numpy as jnp
from jax import lax
from jax.experimental import pallas as pl
from jax.experimental.pallas import tpu as pltpu
from jax.sharding import PartitionSpec as P

CHUNK = 32
UNROLL = 8
STEPS = 32767.0
WAYS = ((1, 1), (1, -1), (-1, 1), (-1, -1), (1, 0), (-1, 0), (0, 1), (0, -1))


def away(by, side):
    return [side + 1] if by > 0 else ([0] if by < 0 else list(range(1, side + 1)))


def edge_places(way, side):
    i, j = WAYS[way]
    return [r * (side + 2) + c for r in away(i, side) for c in away(j, side)]


def edge_start(way, side):
    return sum(len(edge_places(w, side)) for w in range(way))


def halo_copies(side):
    copies = []
    for way, (i, j) in enumerate(WAYS):
        sent = [side - 1] if i > 0 else ([0] if i < 0 else list(range(side)))
        held = away(-i, side)
        col = side - 1 if j > 0 else 0
        for r, h in zip(sent, held):
            copies.append((way, r, col, h * (side + 2) + away(-j, side)[0], 1 if j else side))
    return copies


def spread(side, lon_count, ids, counts):
    cycle = side * lon_count
    if cycle & (cycle - 1) == 0:
        row = lax.shift_right_logical(ids, cycle.bit_length() - 1)
        col = ids & (cycle - 1)
    else:
        row = lax.div(ids, cycle)
        col = ids - row * cycle
    ext_row = row - lax.axis_index("lat") * side + 1
    ext_col = col - lax.axis_index("lon") * side + 1
    ext_col = jnp.where(ext_col < 0, ext_col + cycle, ext_col)
    ext_col = jnp.where(ext_col >= cycle, ext_col - cycle, ext_col)
    width = side + 2
    slot = lax.broadcasted_iota(jnp.int32, ids.shape, 0)
    return jnp.where(slot < counts, ext_row * width + ext_col, width * width)


def adjoint_kernel(
    side, lon_count, ids_ref, counts_ref, cot_ref, w_ref, own_ref, code_ref, scale_ref, place_ref,
    acc, cot, w_vmem, ids, counts, live, place, of_target, of_slot, w_sems, sems,
):
    targets, slots = w_ref.shape[2:4]
    cells = w_ref.shape[4]
    width = side + 2
    trash = width * width
    live_copy = pltpu.make_async_copy(counts_ref.at[0], live, sems.at[0])
    counts_copy = pltpu.make_async_copy(counts_ref.at[0], counts, sems.at[1])
    ids_copy = pltpu.make_async_copy(ids_ref.at[0, 0], ids, sems.at[2])
    cot_copy = pltpu.make_async_copy(cot_ref.at[0, 0], cot, sems.at[3])
    live_copy.start()
    counts_copy.start()
    ids_copy.start()
    cot_copy.start()
    live_copy.wait()

    def pairs_of(t):
        return lax.shift_right_logical(live[0, t] + 1, 1)

    def weight_copy(t, at):
        n = pairs_of(t) * 2
        return pltpu.make_async_copy(
            w_ref.at[0, 0, t, pl.ds(0, n)], w_vmem.at[pl.ds(at * 2, n)], w_sems.at[t]
        )

    def issue(t, at):
        n = pairs_of(t)

        @pl.when(n > 0)
        def _():
            weight_copy(t, at).start()

        for j in range(slots // 2):
            of_target[at + j] = t
            of_slot[at + j] = 2 * j
        return at + n

    total = lax.fori_loop(0, targets, issue, 0)
    counts_copy.wait()
    ids_copy.wait()
    place_ref[...] = spread(side, lon_count, ids[...], counts[...])
    place_copy = pltpu.make_async_copy(place_ref, place, sems.at[4])
    place_copy.start()
    acc[...] = jnp.zeros_like(acc)
    cot_copy.wait()
    place_copy.wait()

    def chunk(c, met):
        base = c * CHUNK
        last = of_target[jnp.minimum(base + CHUNK, total) - 1]

        def meet(t, at):
            n = pairs_of(t)

            @pl.when(n > 0)
            def _():
                weight_copy(t, at).wait()

            return at

        lax.fori_loop(met, last + 1, meet, 0)
        for u in range(CHUNK):
            at = base + u
            there = at < total
            t = jnp.where(there, of_target[at], 0)
            k = jnp.where(there, of_slot[at], 0)
            both = lax.dot_general(
                cot[t],
                w_vmem[pl.ds(2 * at, 2)].reshape(2 * cells, cells),
                (((1,), (1,)), ((), ())),
                preferred_element_type=jnp.float32,
            )
            for m in range(2):
                to = jnp.where(there, place[k + m, t], trash)
                acc[to] += both[:, m * cells:(m + 1) * cells]
        return last + 1

    lax.fori_loop(0, lax.div(total + (CHUNK - 1), CHUNK), chunk, 0)
    for r in range(side):
        for c in range(side):
            own_ref[r, c] = acc[(r + 1) * width + c + 1]
    for way in range(len(WAYS)):
        for n, p in enumerate(edge_places(way, side)):
            block = acc[p]
            most = jnp.max(jnp.abs(block), axis=0, keepdims=True)
            steps = jnp.where(most > 0, STEPS / most, 0.0)
            at = edge_start(way, side) + n
            scale_ref[at] = most * (1.0 / STEPS)
            code_ref[at] = jnp.round(block * steps).astype(jnp.int32).astype(jnp.int16)


def exchange_kernel(
    sizes, place_ref, own_ref, part_ref, code_ref, scale_ref, w_ref, ocean_ref, out_ref,
    acc, ext, codes, scales, place, w_vmem, w_sems, sems, halo_send, halo_recv, code_send, code_recv,
    scale_send, scale_recv, relay_send, relay_recv,
):
    lats, lons = sizes
    lat, lon = lax.axis_index("lat"), lax.axis_index("lon")
    side = out_ref.shape[0]
    width = side + 2
    targets, slots = w_vmem.shape[:2]
    cells = w_vmem.shape[2]
    barrier = pltpu.get_barrier_semaphore()

    def peer(i, j):
        return (lat + i, lax.rem(lon + j + lons, lons))

    def sends(i):
        return (lat + i >= 0) & (lat + i < lats)

    def gets(i):
        return (lat - i >= 0) & (lat - i < lats)

    for i, j in WAYS:
        @pl.when(sends(i))
        def _(i=i, j=j):
            pl.semaphore_signal(
                barrier, inc=1, device_id=peer(i, j), device_id_type=pl.DeviceIdType.MESH
            )

    def weights_of(t):
        return pltpu.make_async_copy(w_ref.at[0, 0, t], w_vmem.at[t], w_sems.at[t])

    place_copy = pltpu.make_async_copy(place_ref, place, sems.at[0])
    place_copy.start()

    @pl.loop(0, targets)
    def _(t):
        weights_of(t).start()

    def inward(j):
        return j == 1 - 2 * lax.rem(lon, 2)

    halos = []
    for n, (way, row, col, to, wide) in enumerate(halo_copies(side)):
        i, j = WAYS[way]
        direct = (lambda ok, j=j: ok & jnp.logical_not(inward(j)), lambda ok, j=j: ok & inward(j))
        send, get = direct if i and j else (lambda ok: ok, lambda ok: ok)
        halos.append((i, j, send(sends(i)), get(gets(i)), pltpu.make_async_remote_copy(
            src_ref=own_ref.at[row, pl.ds(col, wide)],
            dst_ref=ext.at[pl.ds(to, wide)],
            send_sem=halo_send.at[n],
            recv_sem=halo_recv.at[n],
            device_id=peer(i, j),
            device_id_type=pl.DeviceIdType.MESH,
        )))
    odd = lax.rem(lon, 2)
    relays = []
    for n, i in enumerate((1, -1)):
        base = away(-i, side)[0] * width
        relays.append((i, pltpu.make_async_remote_copy(
            src_ref=ext.at[pl.ds(base + side - (side - 1) * odd, 1)],
            dst_ref=ext.at[pl.ds(base + (side + 1) * odd, 1)],
            send_sem=relay_send.at[n],
            recv_sem=relay_recv.at[n],
            device_id=(lat, lon + 1 - 2 * odd),
            device_id_type=pl.DeviceIdType.MESH,
        )))
    folds = []
    for way, (i, j) in enumerate(WAYS):
        span = pl.ds(edge_start(way, side), len(edge_places(way, side)))
        for from_ref, to_ref, send, recv in (
            (scale_ref, scales, scale_send, scale_recv), (code_ref, codes, code_send, code_recv)
        ):
            folds.append((i, pltpu.make_async_remote_copy(
                src_ref=from_ref.at[span],
                dst_ref=to_ref.at[span],
                send_sem=send.at[way],
                recv_sem=recv.at[way],
                device_id=peer(i, j),
                device_id_type=pl.DeviceIdType.MESH,
            )))
    north = (lat > 0).astype(jnp.int32)
    south = (lat < lats - 1).astype(jnp.int32)
    pl.semaphore_wait(barrier, 2 + 3 * north + 3 * south)
    halos = [h for h in halos if not h[1]] + [h for h in halos if h[0] and h[1]] + [
        h for h in halos if not h[0]
    ]
    for _, _, send, _, copy in halos:
        pl.when(send)(copy.start)
    acc[...] = part_ref[...]
    for r in range(side):
        for c in range(side):
            ext[(r + 1) * width + c + 1] = own_ref[r, c]
    blank = jnp.zeros(ext.shape[1:], ext.dtype)
    ext[width * width] = blank
    for i, row in ((1, 0), (-1, side + 1)):
        @pl.when(jnp.logical_not(gets(i)))
        def _(row=row):
            for c in range(width):
                ext[row * width + c] = blank
    place_copy.wait()
    for i, j, _, get, copy in halos:
        pl.when(get)(copy.wait_recv)
        if not j:
            pl.when(get)([copy for at, copy in relays if at == i][0].start)
    for i, copy in relays:
        pl.when(gets(i))(copy.wait_recv)
    for i, copy in folds:
        pl.when(sends(i))(copy.start)

    @pl.loop(0, targets // UNROLL)
    def _(g):
        for u in range(UNROLL):
            weights_of(g * UNROLL + u).wait()
        for u in range(UNROLL):
            t = g * UNROLL + u
            picked = jnp.concatenate([ext[place[k, t]] for k in range(slots)], axis=1)
            blocks = w_vmem[t].reshape(slots * cells, w_vmem.shape[3])
            total = jnp.dot(picked, blocks, preferred_element_type=jnp.float32)
            ocean_ref[0, 0, t] = total.astype(ocean_ref.dtype)

    for i, copy in folds:
        pl.when(gets(i))(copy.wait_recv)
    for way, (i, j) in enumerate(WAYS):
        rows = [r - 1 for r in away(-i, side)] if i == 0 else [0 if i > 0 else side - 1]
        cols = [c - 1 for c in away(-j, side)] if j == 0 else [0 if j > 0 else side - 1]

        @pl.when(gets(i))
        def _(way=way, rows=rows, cols=cols):
            for n, (r, c) in enumerate((r, c) for r in rows for c in cols):
                at = edge_start(way, side) + n
                acc[r, c] += codes[at].astype(jnp.int32).astype(jnp.float32) * scales[at]

    out_ref[...] = acc[...].astype(out_ref.dtype)
    for _, _, send, _, copy in halos:
        pl.when(send)(copy.wait_send)
    for i, copy in relays:
        pl.when(gets(i))(copy.wait_send)
    for i, copy in folds:
        pl.when(sends(i))(copy.wait_send)


def body(increment, cotangent, weights, source_ids, counts):
    side, _, levels, cells = increment.shape
    sizes = lax.axis_size("lat"), lax.axis_size("lon")
    vmem = pl.BlockSpec(memory_space=pltpu.VMEM)
    hbm = pl.BlockSpec(memory_space=pltpu.HBM)
    targets, slots = weights.shape[2:4]
    width = side + 2
    flat = (width * width + 1, levels, cells)
    edges = edge_start(len(WAYS), side)
    hops = len(halo_copies(side))
    pairs = targets * slots // 2
    cost = pl.CostEstimate(
        flops=2 * targets * slots * levels * cells * cells,
        bytes_accessed=weights.size * 2,
        transcendentals=0,
    )
    limit = 50 * 1024 * 1024
    own, code, scale, place = pl.pallas_call(
        functools.partial(adjoint_kernel, side, sizes[1]),
        out_shape=[
            jax.ShapeDtypeStruct(increment.shape, jnp.float32),
            jax.ShapeDtypeStruct((edges, levels, cells), jnp.int16),
            jax.ShapeDtypeStruct((edges, 1, cells), jnp.float32),
            jax.ShapeDtypeStruct((slots, targets), jnp.int32),
        ],
        in_specs=[hbm, hbm, hbm, hbm],
        out_specs=[vmem, vmem, vmem, vmem],
        scratch_shapes=[
            pltpu.VMEM(flat, jnp.float32),
            pltpu.VMEM(cotangent.shape[2:], cotangent.dtype),
            pltpu.VMEM((targets * slots + 2 * CHUNK, cells, weights.shape[5]), weights.dtype),
            pltpu.VMEM((slots, targets), jnp.int32),
            pltpu.VMEM((1, targets), jnp.int32),
            pltpu.SMEM((1, targets), jnp.int32),
            pltpu.SMEM((slots, targets), jnp.int32),
            pltpu.SMEM((pairs + CHUNK + slots,), jnp.int32),
            pltpu.SMEM((pairs + CHUNK + slots,), jnp.int32),
            pltpu.SemaphoreType.DMA((targets,)),
            pltpu.SemaphoreType.DMA((5,)),
        ],
        compiler_params=pltpu.CompilerParams(vmem_limit_bytes=limit),
        cost_estimate=cost,
        name="adjoint",
    )(*[pltpu.with_memory_space_constraint(x, pltpu.HBM) for x in (jnp.swapaxes(source_ids, 2, 3), counts, cotangent, weights)])
    ways = len(WAYS)
    return pl.pallas_call(
        functools.partial(exchange_kernel, sizes),
        out_shape=[
            jax.ShapeDtypeStruct(cotangent.shape, jnp.bfloat16),
            jax.ShapeDtypeStruct(increment.shape, jnp.bfloat16),
        ],
        in_specs=[vmem, vmem, vmem, vmem, vmem, hbm],
        out_specs=[vmem, vmem],
        scratch_shapes=[
            pltpu.VMEM(increment.shape, jnp.float32),
            pltpu.VMEM(flat, increment.dtype),
            pltpu.VMEM((edges, levels, cells), jnp.int16),
            pltpu.VMEM((edges, 1, cells), jnp.float32),
            pltpu.SMEM((slots, targets), jnp.int32),
            pltpu.VMEM(weights.shape[2:], weights.dtype),
            pltpu.SemaphoreType.DMA((targets,)),
            pltpu.SemaphoreType.DMA((1,)),
        ] + [pltpu.SemaphoreType.DMA((hops,))] * 2 + [pltpu.SemaphoreType.DMA((ways,))] * 4
        + [pltpu.SemaphoreType.DMA((2,))] * 2,
        compiler_params=pltpu.CompilerParams(
            collective_id=0, has_side_effects=True, vmem_limit_bytes=limit
        ),
        cost_estimate=cost,
        name="exchange",
    )(place, increment, own, code, scale, weights)


def solution(mesh):
    placed = (
        P("lat", "lon", None, None),
        P("lat", "lon", None, None, None),
        P("lat", "lon", None, None, None, None),
        P("lat", "lon", None, None),
        P("lat", "lon", None),
    )
    return jax.shard_map(
        body,
        mesh=mesh,
        in_specs=placed,
        out_specs=(P("lat", "lon", None, None, None), P("lat", "lon", None, None)),
        check_vma=False,
    )
```

```python
import functools

import jax
import jax.numpy as jnp
from jax import lax
from jax.experimental import pallas as pl
from jax.experimental.pallas import tpu as pltpu
from jax.sharding import PartitionSpec as P

CHUNK = 32
HEAD = 4
SHARES = 8
UNROLL = 8
STEPS = 32767.0
WAYS = ((1, 1), (1, -1), (-1, 1), (-1, -1), (1, 0), (-1, 0), (0, 1), (0, -1))


def away(by, side):
    return [side + 1] if by > 0 else ([0] if by < 0 else list(range(1, side + 1)))


def edge_places(way, side):
    i, j = WAYS[way]
    return [r * (side + 2) + c for r in away(i, side) for c in away(j, side)]


def edge_start(way, side):
    return sum(len(edge_places(w, side)) for w in range(way))


def halo_copies(side):
    copies = []
    for way, (i, j) in enumerate(WAYS):
        sent = [side - 1] if i > 0 else ([0] if i < 0 else list(range(side)))
        held = away(-i, side)
        col = side - 1 if j > 0 else 0
        for r, h in zip(sent, held):
            copies.append((way, r, col, h * (side + 2) + away(-j, side)[0], 1 if j else side))
    return copies


def spread(side, lon_count, ids, counts):
    cycle = side * lon_count
    if cycle & (cycle - 1) == 0:
        row = lax.shift_right_logical(ids, cycle.bit_length() - 1)
        col = ids & (cycle - 1)
    else:
        row = lax.div(ids, cycle)
        col = ids - row * cycle
    ext_row = row - lax.axis_index("lat") * side + 1
    ext_col = col - lax.axis_index("lon") * side + 1
    ext_col = jnp.where(ext_col < 0, ext_col + cycle, ext_col)
    ext_col = jnp.where(ext_col >= cycle, ext_col - cycle, ext_col)
    width = side + 2
    slot = lax.broadcasted_iota(jnp.int32, ids.shape, 0)
    return jnp.where(slot < counts, ext_row * width + ext_col, width * width)


def adjoint_kernel(
    side, lon_count, ids_ref, counts_ref, cot_ref, w_ref, part_ref, place_ref,
    cot, w_vmem, ids, counts, live, place, of_target, of_slot, w_sems, sems,
):
    targets, slots = w_ref.shape[2:4]
    cells = w_ref.shape[4]
    trash = part_ref.shape[0] - 1
    live_copy = pltpu.make_async_copy(counts_ref.at[0], live, sems.at[0])
    counts_copy = pltpu.make_async_copy(counts_ref.at[0], counts, sems.at[1])
    ids_copy = pltpu.make_async_copy(ids_ref.at[0, 0], ids, sems.at[2])
    cot_copy = pltpu.make_async_copy(cot_ref.at[0, 0], cot, sems.at[3])
    live_copy.start()
    counts_copy.start()
    ids_copy.start()

    def weight_copy(t, n):
        return pltpu.make_async_copy(
            w_ref.at[0, 0, t, pl.ds(0, n)], w_vmem.at[pl.ds(t * slots, n)], w_sems.at[t]
        )

    for t in range(HEAD):
        weight_copy(t, slots).start()
    cot_copy.start()
    part_ref[...] = jnp.zeros_like(part_ref)
    live_copy.wait()

    def pairs_of(t):
        return lax.shift_right_logical(live[0, t] + 1, 1)

    def enlist(t, at):
        for j in range(slots // 2):
            of_target[at + j] = t
            of_slot[at + j] = 2 * j
        return at + pairs_of(t)

    def issue(t, at):
        n = pairs_of(t)

        @pl.when(n > 0)
        def _():
            weight_copy(t, n * 2).start()

        return enlist(t, at)

    total = lax.fori_loop(HEAD, targets, issue, lax.fori_loop(0, HEAD, enlist, 0))
    counts_copy.wait()
    ids_copy.wait()
    place_ref[...] = spread(side, lon_count, ids[...], counts[...])
    place_copy = pltpu.make_async_copy(place_ref, place, sems.at[4])
    place_copy.start()
    cot_copy.wait()
    place_copy.wait()
    for t in range(HEAD):
        weight_copy(t, slots).wait()

    def chunk(c, met):
        base = c * CHUNK
        last = of_target[jnp.minimum(base + CHUNK, total) - 1]

        def meet(t, carry):
            n = pairs_of(t)

            @pl.when(n > 0)
            def _():
                weight_copy(t, n * 2).wait()

            return carry

        lax.fori_loop(met, last + 1, meet, 0)
        for u in range(CHUNK):
            there = base + u < total
            t = jnp.where(there, of_target[base + u], 0)
            k = jnp.where(there, of_slot[base + u], 0)
            both = lax.dot_general(
                cot[t],
                w_vmem[pl.ds(t * slots + k, 2)].reshape(2 * cells, cells),
                (((1,), (1,)), ((), ())),
                preferred_element_type=jnp.float32,
            )
            for m in range(2):
                to = jnp.where(there, place[k + m, t], trash)
                part_ref[to] += both[:, m * cells:(m + 1) * cells]
        return jnp.maximum(met, last + 1)

    lax.fori_loop(0, lax.div(total + (CHUNK - 1), CHUNK), chunk, HEAD)


def encode(block, code_ref, scale_ref, at):
    most = jnp.max(jnp.abs(block), axis=0, keepdims=True)
    steps = jnp.where(most > 0, STEPS / most, 0.0)
    scale_ref[at] = most * (1.0 / STEPS)
    code_ref[at] = jnp.round(block * steps).astype(jnp.int32).astype(jnp.int16)


def exchange_kernel(
    sizes, place_ref, own_ref, part_ref, w_ref, ocean_ref, out_ref,
    code_ref, scale_ref, codes, scales, nears, acc, ext, place, w_vmem, w_sems, sems, halo_send, halo_recv, code_send, code_recv,
    scale_send, scale_recv, relay_send, relay_recv, near_send, near_recv,
):
    lats, lons = sizes
    lat, lon = lax.axis_index("lat"), lax.axis_index("lon")
    side = out_ref.shape[0]
    width = side + 2
    targets, slots = w_vmem.shape[:2]
    cells = w_vmem.shape[2]
    barrier = pltpu.get_barrier_semaphore()

    def peer(i, j):
        return (lat + i, lax.rem(lon + j + lons, lons))

    def sends(i):
        return (lat + i >= 0) & (lat + i < lats)

    def gets(i):
        return (lat - i >= 0) & (lat - i < lats)

    for i, j in WAYS:
        @pl.when(sends(i))
        def _(i=i, j=j):
            pl.semaphore_signal(
                barrier, inc=1, device_id=peer(i, j), device_id_type=pl.DeviceIdType.MESH
            )

    def weights_of(t):
        return pltpu.make_async_copy(w_ref.at[0, 0, t], w_vmem.at[t], w_sems.at[t])

    place_copy = pltpu.make_async_copy(place_ref, place, sems.at[0])
    place_copy.start()

    @pl.loop(0, targets)
    def _(t):
        weights_of(t).start()

    def inward(j):
        return j == 1 - 2 * lax.rem(lon, 2)

    halos = []
    for n, (way, row, col, to, wide) in enumerate(halo_copies(side)):
        i, j = WAYS[way]
        direct = (lambda ok, j=j: ok & jnp.logical_not(inward(j)), lambda ok, j=j: ok & inward(j))
        send, get = direct if i and j else (lambda ok: ok, lambda ok: ok)
        halos.append((i, j, send(sends(i)), get(gets(i)), pltpu.make_async_remote_copy(
            src_ref=own_ref.at[row, pl.ds(col, wide)],
            dst_ref=ext.at[pl.ds(to, wide)],
            send_sem=halo_send.at[n],
            recv_sem=halo_recv.at[n],
            device_id=peer(i, j),
            device_id_type=pl.DeviceIdType.MESH,
        )))
    odd = lax.rem(lon, 2)
    relays = []
    for n, i in enumerate((1, -1)):
        base = away(-i, side)[0] * width
        relays.append((i, pltpu.make_async_remote_copy(
            src_ref=ext.at[pl.ds(base + side - (side - 1) * odd, 1)],
            dst_ref=ext.at[pl.ds(base + (side + 1) * odd, 1)],
            send_sem=relay_send.at[n],
            recv_sem=relay_recv.at[n],
            device_id=(lat, lon + 1 - 2 * odd),
            device_id_type=pl.DeviceIdType.MESH,
        )))
    folds = []
    for way, (i, j) in enumerate(WAYS):
        span = pl.ds(edge_start(way, side), len(edge_places(way, side)))
        send, get = sends(i), gets(i)
        if i and j:
            send, get = send & jnp.logical_not(inward(j)), get & inward(j)
        for from_ref, to_ref, out, back in (
            (scale_ref, scales, scale_send, scale_recv), (code_ref, codes, code_send, code_recv)
        ):
            folds.append((i, j, send, get, pltpu.make_async_remote_copy(
                src_ref=from_ref.at[span],
                dst_ref=to_ref.at[span],
                send_sem=out.at[way],
                recv_sem=back.at[way],
                device_id=peer(i, j),
                device_id_type=pl.DeviceIdType.MESH,
            )))
    partner = (lat, lon + 1 - 2 * odd)
    near = []
    for n, i in enumerate((1, -1)):
        far = away(i, side)[0] * width + (side + 1) * (1 - odd)
        near.append((i, pltpu.make_async_remote_copy(
            src_ref=part_ref.at[pl.ds(far, 1)],
            dst_ref=nears.at[pl.ds(n, 1)],
            send_sem=near_send.at[n],
            recv_sem=near_recv.at[n],
            device_id=partner,
            device_id_type=pl.DeviceIdType.MESH,
        )))
    for way, (i, j) in enumerate(WAYS):
        for n, p in enumerate(edge_places(way, side)):
            if j:
                encode(part_ref[p], code_ref, scale_ref, edge_start(way, side) + n)
    north = (lat > 0).astype(jnp.int32)
    south = (lat < lats - 1).astype(jnp.int32)
    pl.semaphore_wait(barrier, 2 + 3 * north + 3 * south)
    halos = [h for h in halos if not h[1]] + [h for h in halos if h[0] and h[1]] + [
        h for h in halos if not h[0]
    ]
    for _, _, send, _, copy in halos:
        pl.when(send)(copy.start)
    for i, copy in near:
        pl.when(sends(i))(copy.start)
    for r in range(side):
        for c in range(side):
            acc[r, c] = part_ref[(r + 1) * width + c + 1]
            ext[(r + 1) * width + c + 1] = own_ref[r, c]
    blank = jnp.zeros(ext.shape[1:], ext.dtype)
    ext[width * width] = blank
    for i, row in ((1, 0), (-1, side + 1)):
        @pl.when(jnp.logical_not(gets(i)))
        def _(row=row):
            for c in range(width):
                ext[row * width + c] = blank
    place_copy.wait()
    for n, (i, copy) in enumerate(near):
        @pl.when(sends(i))
        def _(n=n, i=i, copy=copy):
            copy.wait_recv()
            way = WAYS.index((i, 0))
            for at, p in enumerate(edge_places(way, side)):
                meets = (1 - odd) * (side - 1) == at
                block = part_ref[p] + jnp.where(meets, nears[n], 0.0)
                encode(block, code_ref, scale_ref, edge_start(way, side) + at)

    for i, j, _, get, copy in halos:
        pl.when(get)(copy.wait_recv)
        if not j:
            pl.when(get)([copy for at, copy in relays if at == i][0].start)
    for i, copy in relays:
        pl.when(gets(i))(copy.wait_recv)
    for _, _, send, _, copy in folds:
        pl.when(send)(copy.start)

    @pl.loop(0, targets // UNROLL)
    def _(g):
        for u in range(UNROLL):
            weights_of(g * UNROLL + u).wait()
        for u in range(UNROLL):
            t = g * UNROLL + u
            picked = jnp.concatenate([ext[place[k, t]] for k in range(slots)], axis=1)
            blocks = w_vmem[t].reshape(slots * cells, w_vmem.shape[3])
            total = jnp.dot(picked, blocks, preferred_element_type=jnp.float32)
            ocean_ref[0, 0, t] = total.astype(ocean_ref.dtype)

    for _, _, _, get, copy in folds:
        pl.when(get)(copy.wait_recv)
    for way, (i, j) in enumerate(WAYS):
        rows = [r - 1 for r in away(-i, side)] if i == 0 else [0 if i > 0 else side - 1]
        cols = [c - 1 for c in away(-j, side)] if j == 0 else [0 if j > 0 else side - 1]

        @pl.when(gets(i) & inward(j) if i and j else gets(i))
        def _(way=way, rows=rows, cols=cols):
            for n, (r, c) in enumerate((r, c) for r in rows for c in cols):
                at = edge_start(way, side) + n
                acc[r, c] += codes[at].astype(jnp.int32).astype(jnp.float32) * scales[at]

    out_ref[...] = acc[...].astype(out_ref.dtype)
    for _, _, send, _, copy in halos:
        pl.when(send)(copy.wait_send)
    for i, copy in relays:
        pl.when(gets(i))(copy.wait_send)
    for i, copy in near:
        pl.when(sends(i))(copy.wait_send)
    for _, _, send, _, copy in folds:
        pl.when(send)(copy.wait_send)


def deliver_kernel(ocean_ref, part_ref, ocean_out, part_out, sems):
    targets = ocean_ref.shape[2]
    step = -(-targets // SHARES)
    copies = [pltpu.make_async_copy(part_ref, part_out, sems.at[SHARES])]
    for n in range(SHARES):
        span = pl.ds(n * step, max(min(step, targets - n * step), 0))
        copies.append(
            pltpu.make_async_copy(ocean_ref.at[0, 0, span], ocean_out.at[0, 0, span], sems.at[n])
        )
    for copy in copies:
        copy.start()
    for copy in copies:
        copy.wait()


def body(increment, cotangent, weights, source_ids, counts):
    side, _, levels, cells = increment.shape
    sizes = lax.axis_size("lat"), lax.axis_size("lon")
    vmem = pl.BlockSpec(memory_space=pltpu.VMEM)
    hbm = pl.BlockSpec(memory_space=pltpu.HBM)
    targets, slots = weights.shape[2:4]
    width = side + 2
    flat = (width * width + 1, levels, cells)
    edges = edge_start(len(WAYS), side)
    hops = len(halo_copies(side))
    pairs = targets * slots // 2
    cost = pl.CostEstimate(
        flops=2 * targets * slots * levels * cells * cells,
        bytes_accessed=weights.size * 2,
        transcendentals=0,
    )
    limit = 50 * 1024 * 1024
    whole, rows, held_counts = (
        pltpu.with_memory_space_constraint(x, pltpu.HBM)
        for x in (weights, jnp.swapaxes(source_ids, 2, 3), counts)
    )
    part, place = pl.pallas_call(
        functools.partial(adjoint_kernel, side, sizes[1]),
        out_shape=[
            jax.ShapeDtypeStruct(flat, jnp.float32),
            jax.ShapeDtypeStruct((slots, targets), jnp.int32),
        ],
        in_specs=[hbm, hbm, hbm, hbm],
        out_specs=[vmem, vmem],
        scratch_shapes=[
            pltpu.VMEM(cotangent.shape[2:], cotangent.dtype),
            pltpu.VMEM((targets * slots, cells, weights.shape[5]), weights.dtype),
            pltpu.VMEM((slots, targets), jnp.int32),
            pltpu.VMEM((1, targets), jnp.int32),
            pltpu.SMEM((1, targets), jnp.int32),
            pltpu.SMEM((slots, targets), jnp.int32),
            pltpu.SMEM((pairs + CHUNK + slots,), jnp.int32),
            pltpu.SMEM((pairs + CHUNK + slots,), jnp.int32),
            pltpu.SemaphoreType.DMA((targets,)),
            pltpu.SemaphoreType.DMA((5,)),
        ],
        compiler_params=pltpu.CompilerParams(vmem_limit_bytes=limit),
        cost_estimate=cost,
        name="adjoint",
    )(rows, held_counts, pltpu.with_memory_space_constraint(cotangent, pltpu.HBM), whole)
    ways = len(WAYS)
    coded = [
        pltpu.VMEM((edges, levels, cells), jnp.int16),
        pltpu.VMEM((edges, 1, cells), jnp.float32),
    ]
    results = [
        jax.ShapeDtypeStruct(cotangent.shape, jnp.bfloat16),
        jax.ShapeDtypeStruct(increment.shape, jnp.bfloat16),
    ]
    ocean, adjoint = pl.pallas_call(
        functools.partial(exchange_kernel, sizes),
        out_shape=results,
        in_specs=[vmem, vmem, vmem, hbm],
        out_specs=[vmem, vmem],
        scratch_shapes=coded + coded + [
            pltpu.VMEM((2, levels, cells), jnp.float32),
            pltpu.VMEM(increment.shape, jnp.float32),
            pltpu.VMEM(flat, increment.dtype),
            pltpu.SMEM((slots, targets), jnp.int32),
            pltpu.VMEM(weights.shape[2:], weights.dtype),
            pltpu.SemaphoreType.DMA((targets,)),
            pltpu.SemaphoreType.DMA((1,)),
        ] + [pltpu.SemaphoreType.DMA((hops,))] * 2 + [pltpu.SemaphoreType.DMA((ways,))] * 4
        + [pltpu.SemaphoreType.DMA((2,))] * 4,
        compiler_params=pltpu.CompilerParams(
            collective_id=0, has_side_effects=True, vmem_limit_bytes=limit
        ),
        cost_estimate=cost,
        name="exchange",
    )(place, increment, part, whole)
    return pl.pallas_call(
        deliver_kernel,
        out_shape=results,
        in_specs=[vmem] * 2,
        out_specs=[hbm] * 2,
        scratch_shapes=[pltpu.SemaphoreType.DMA((SHARES + 1,))],
        compiler_params=pltpu.CompilerParams(vmem_limit_bytes=limit),
        name="deliver",
    )(ocean, adjoint)


def solution(mesh):
    placed = (
        P("lat", "lon", None, None),
        P("lat", "lon", None, None, None),
        P("lat", "lon", None, None, None, None),
        P("lat", "lon", None, None),
        P("lat", "lon", None),
    )
    return jax.shard_map(
        body,
        mesh=mesh,
        in_specs=placed,
        out_specs=(P("lat", "lon", None, None, None), P("lat", "lon", None, None)),
        check_vma=False,
    )
```

```python
import functools

import jax
import jax.numpy as jnp
from jax import lax
from jax.experimental import pallas as pl
from jax.experimental.pallas import tpu as pltpu
from jax.sharding import PartitionSpec as P

CHUNK = 32
HEAD = 4
SHARES = 8
UNROLL = 10
STEPS = 32767.0
WAYS = ((1, 1), (1, -1), (-1, 1), (-1, -1), (1, 0), (-1, 0), (0, 1), (0, -1))


def away(by, side):
    return [side + 1] if by > 0 else ([0] if by < 0 else list(range(1, side + 1)))


def edge_places(way, side):
    i, j = WAYS[way]
    return [r * (side + 2) + c for r in away(i, side) for c in away(j, side)]


def edge_start(way, side):
    return sum(len(edge_places(w, side)) for w in range(way))


def halo_copies(side):
    copies = []
    for way, (i, j) in enumerate(WAYS):
        sent = [side - 1] if i > 0 else ([0] if i < 0 else list(range(side)))
        held = away(-i, side)
        col = side - 1 if j > 0 else 0
        for r, h in zip(sent, held):
            copies.append((way, r, col, h * (side + 2) + away(-j, side)[0], 1 if j else side))
    return copies


def spread(side, lon_count, ids, counts):
    cycle = side * lon_count
    if cycle & (cycle - 1) == 0:
        row = lax.shift_right_logical(ids, cycle.bit_length() - 1)
        col = ids & (cycle - 1)
    else:
        row = lax.div(ids, cycle)
        col = ids - row * cycle
    ext_row = row - lax.axis_index("lat") * side + 1
    ext_col = col - lax.axis_index("lon") * side + 1
    ext_col = jnp.where(ext_col < 0, ext_col + cycle, ext_col)
    ext_col = jnp.where(ext_col >= cycle, ext_col - cycle, ext_col)
    width = side + 2
    slot = lax.broadcasted_iota(jnp.int32, ids.shape, 0)
    return jnp.where(slot < counts, ext_row * width + ext_col, width * width)


def adjoint_kernel(
    side, lon_count, ids_ref, counts_ref, cot_ref, w_ref, part_ref, place_ref,
    cot, w_vmem, ids, counts, live, place, of_target, of_slot, w_sems, sems,
):
    targets, slots = w_ref.shape[2:4]
    cells = w_ref.shape[4]
    trash = part_ref.shape[0] - 1
    live_copy = pltpu.make_async_copy(counts_ref.at[0], live, sems.at[0])
    counts_copy = pltpu.make_async_copy(counts_ref.at[0], counts, sems.at[1])
    ids_copy = pltpu.make_async_copy(ids_ref.at[0, 0], ids, sems.at[2])
    cot_copy = pltpu.make_async_copy(cot_ref.at[0, 0], cot, sems.at[3])
    live_copy.start()
    counts_copy.start()
    ids_copy.start()

    def weight_copy(t, n):
        return pltpu.make_async_copy(
            w_ref.at[0, 0, t, pl.ds(0, n)], w_vmem.at[pl.ds(t * slots, n)], w_sems.at[t]
        )

    for t in range(HEAD):
        weight_copy(t, slots).start()
    cot_copy.start()
    part_ref[...] = jnp.zeros_like(part_ref)
    live_copy.wait()

    def pairs_of(t):
        return lax.shift_right_logical(live[0, t] + 1, 1)

    def enlist(t, at):
        for j in range(slots // 2):
            of_target[at + j] = t
            of_slot[at + j] = 2 * j
        return at + pairs_of(t)

    def issue(t, at):
        n = pairs_of(t)

        @pl.when(n > 0)
        def _():
            weight_copy(t, n * 2).start()

        return enlist(t, at)

    total = lax.fori_loop(HEAD, targets, issue, lax.fori_loop(0, HEAD, enlist, 0))
    counts_copy.wait()
    ids_copy.wait()
    place_ref[...] = spread(side, lon_count, ids[...], counts[...])
    place_copy = pltpu.make_async_copy(place_ref, place, sems.at[4])
    place_copy.start()
    cot_copy.wait()
    place_copy.wait()
    for t in range(HEAD):
        weight_copy(t, slots).wait()

    def chunk(c, met):
        base = c * CHUNK
        last = of_target[jnp.minimum(base + CHUNK, total) - 1]

        def meet(t, carry):
            n = pairs_of(t)

            @pl.when(n > 0)
            def _():
                weight_copy(t, n * 2).wait()

            return carry

        lax.fori_loop(met, last + 1, meet, 0)
        for u in range(CHUNK):
            there = base + u < total
            t = jnp.where(there, of_target[base + u], 0)
            k = jnp.where(there, of_slot[base + u], 0)
            both = lax.dot_general(
                cot[t],
                w_vmem[pl.ds(t * slots + k, 2)].reshape(2 * cells, cells),
                (((1,), (1,)), ((), ())),
                preferred_element_type=jnp.float32,
            )
            for m in range(2):
                to = jnp.where(there, place[k + m, t], trash)
                part_ref[to] += both[:, m * cells:(m + 1) * cells]
        return jnp.maximum(met, last + 1)

    lax.fori_loop(0, lax.div(total + (CHUNK - 1), CHUNK), chunk, HEAD)


def encode(block, code_ref, scale_ref, at):
    most = jnp.max(jnp.abs(block), axis=0, keepdims=True)
    steps = jnp.where(most > 0, STEPS / most, 0.0)
    scale_ref[at] = most * (1.0 / STEPS)
    code_ref[at] = jnp.round(block * steps).astype(jnp.int32).astype(jnp.int16)


def exchange_kernel(
    sizes, place_ref, own_ref, part_ref, w_ref, ocean_ref, out_ref,
    code_ref, scale_ref, codes, scales, nears, acc, ext, place, w_vmem, w_sems, sems, halo_send, halo_recv, code_send, code_recv,
    scale_send, scale_recv, relay_send, relay_recv, near_send, near_recv,
):
    lats, lons = sizes
    lat, lon = lax.axis_index("lat"), lax.axis_index("lon")
    side = out_ref.shape[0]
    width = side + 2
    targets, slots = w_vmem.shape[:2]
    cells = w_vmem.shape[2]
    barrier = pltpu.get_barrier_semaphore()

    def peer(i, j):
        return (lat + i, lax.rem(lon + j + lons, lons))

    def sends(i):
        return (lat + i >= 0) & (lat + i < lats)

    def gets(i):
        return (lat - i >= 0) & (lat - i < lats)

    for i, j in WAYS:
        @pl.when(sends(i))
        def _(i=i, j=j):
            pl.semaphore_signal(
                barrier, inc=1, device_id=peer(i, j), device_id_type=pl.DeviceIdType.MESH
            )

    def weights_of(t):
        return pltpu.make_async_copy(w_ref.at[0, 0, t], w_vmem.at[t], w_sems.at[t])

    place_copy = pltpu.make_async_copy(place_ref, place, sems.at[0])
    place_copy.start()

    @pl.loop(0, targets)
    def _(t):
        weights_of(t).start()

    def inward(j):
        return j == 1 - 2 * lax.rem(lon, 2)

    halos = []
    for n, (way, row, col, to, wide) in enumerate(halo_copies(side)):
        i, j = WAYS[way]
        direct = (lambda ok, j=j: ok & jnp.logical_not(inward(j)), lambda ok, j=j: ok & inward(j))
        send, get = direct if i and j else (lambda ok: ok, lambda ok: ok)
        halos.append((i, j, send(sends(i)), get(gets(i)), pltpu.make_async_remote_copy(
            src_ref=own_ref.at[row, pl.ds(col, wide)],
            dst_ref=ext.at[pl.ds(to, wide)],
            send_sem=halo_send.at[n],
            recv_sem=halo_recv.at[n],
            device_id=peer(i, j),
            device_id_type=pl.DeviceIdType.MESH,
        )))
    odd = lax.rem(lon, 2)
    relays = []
    for n, i in enumerate((1, -1)):
        base = away(-i, side)[0] * width
        relays.append((i, pltpu.make_async_remote_copy(
            src_ref=ext.at[pl.ds(base + side - (side - 1) * odd, 1)],
            dst_ref=ext.at[pl.ds(base + (side + 1) * odd, 1)],
            send_sem=relay_send.at[n],
            recv_sem=relay_recv.at[n],
            device_id=(lat, lon + 1 - 2 * odd),
            device_id_type=pl.DeviceIdType.MESH,
        )))
    folds = []
    for way, (i, j) in enumerate(WAYS):
        span = pl.ds(edge_start(way, side), len(edge_places(way, side)))
        send, get = sends(i), gets(i)
        if i and j:
            send, get = send & jnp.logical_not(inward(j)), get & inward(j)
        for from_ref, to_ref, out, back in (
            (scale_ref, scales, scale_send, scale_recv), (code_ref, codes, code_send, code_recv)
        ):
            folds.append((i, j, send, get, pltpu.make_async_remote_copy(
                src_ref=from_ref.at[span],
                dst_ref=to_ref.at[span],
                send_sem=out.at[way],
                recv_sem=back.at[way],
                device_id=peer(i, j),
                device_id_type=pl.DeviceIdType.MESH,
            )))
    partner = (lat, lon + 1 - 2 * odd)
    near = []
    for n, i in enumerate((1, -1)):
        far = away(i, side)[0] * width + (side + 1) * (1 - odd)
        near.append((i, pltpu.make_async_remote_copy(
            src_ref=part_ref.at[pl.ds(far, 1)],
            dst_ref=nears.at[pl.ds(n, 1)],
            send_sem=near_send.at[n],
            recv_sem=near_recv.at[n],
            device_id=partner,
            device_id_type=pl.DeviceIdType.MESH,
        )))
    north = (lat > 0).astype(jnp.int32)
    south = (lat < lats - 1).astype(jnp.int32)
    pl.semaphore_wait(barrier, 2 + 3 * north + 3 * south)
    halos = [h for h in halos if not h[1]] + [h for h in halos if h[0] and h[1]] + [
        h for h in halos if not h[0]
    ]
    for _, _, send, _, copy in halos:
        pl.when(send)(copy.start)
    for i, copy in near:
        pl.when(sends(i))(copy.start)
    for way, (i, j) in enumerate(WAYS):
        for n, p in enumerate(edge_places(way, side)):
            if j:
                encode(part_ref[p], code_ref, scale_ref, edge_start(way, side) + n)
    for r in range(side):
        for c in range(side):
            acc[r, c] = part_ref[(r + 1) * width + c + 1]
            ext[(r + 1) * width + c + 1] = own_ref[r, c]
    blank = jnp.zeros(ext.shape[1:], ext.dtype)
    ext[width * width] = blank
    for i, row in ((1, 0), (-1, side + 1)):
        @pl.when(jnp.logical_not(gets(i)))
        def _(row=row):
            for c in range(width):
                ext[row * width + c] = blank
    place_copy.wait()
    for n, (i, copy) in enumerate(near):
        @pl.when(sends(i))
        def _(n=n, i=i, copy=copy):
            copy.wait_recv()
            way = WAYS.index((i, 0))
            for at, p in enumerate(edge_places(way, side)):
                meets = (1 - odd) * (side - 1) == at
                block = part_ref[p] + jnp.where(meets, nears[n], 0.0)
                encode(block, code_ref, scale_ref, edge_start(way, side) + at)

    for i, j, _, get, copy in halos:
        pl.when(get)(copy.wait_recv)
        if not j:
            pl.when(get)([copy for at, copy in relays if at == i][0].start)
    for i, copy in relays:
        pl.when(gets(i))(copy.wait_recv)
    for _, _, send, _, copy in folds:
        pl.when(send)(copy.start)

    @pl.loop(0, targets // UNROLL)
    def _(g):
        for u in range(UNROLL):
            weights_of(g * UNROLL + u).wait()
        for u in range(UNROLL):
            t = g * UNROLL + u
            picked = jnp.concatenate([ext[place[k, t]] for k in range(slots)], axis=1)
            blocks = w_vmem[t].reshape(slots * cells, w_vmem.shape[3])
            total = jnp.dot(picked, blocks, preferred_element_type=jnp.float32)
            ocean_ref[0, 0, t] = total.astype(ocean_ref.dtype)

    for _, _, _, get, copy in folds:
        pl.when(get)(copy.wait_recv)
    for way, (i, j) in enumerate(WAYS):
        rows = [r - 1 for r in away(-i, side)] if i == 0 else [0 if i > 0 else side - 1]
        cols = [c - 1 for c in away(-j, side)] if j == 0 else [0 if j > 0 else side - 1]

        @pl.when(gets(i) & inward(j) if i and j else gets(i))
        def _(way=way, rows=rows, cols=cols):
            for n, (r, c) in enumerate((r, c) for r in rows for c in cols):
                at = edge_start(way, side) + n
                acc[r, c] += codes[at].astype(jnp.int32).astype(jnp.float32) * scales[at]

    out_ref[...] = acc[...].astype(out_ref.dtype)
    for _, _, send, _, copy in halos:
        pl.when(send)(copy.wait_send)
    for i, copy in relays:
        pl.when(gets(i))(copy.wait_send)
    for i, copy in near:
        pl.when(sends(i))(copy.wait_send)
    for _, _, send, _, copy in folds:
        pl.when(send)(copy.wait_send)


def deliver_kernel(ocean_ref, part_ref, ocean_out, part_out, sems):
    targets = ocean_ref.shape[2]
    step = -(-targets // SHARES)
    copies = [pltpu.make_async_copy(part_ref, part_out, sems.at[SHARES])]
    for n in range(SHARES):
        span = pl.ds(n * step, max(min(step, targets - n * step), 0))
        copies.append(
            pltpu.make_async_copy(ocean_ref.at[0, 0, span], ocean_out.at[0, 0, span], sems.at[n])
        )
    for copy in copies:
        copy.start()
    for copy in copies:
        copy.wait()


def body(increment, cotangent, weights, source_ids, counts):
    side, _, levels, cells = increment.shape
    sizes = lax.axis_size("lat"), lax.axis_size("lon")
    vmem = pl.BlockSpec(memory_space=pltpu.VMEM)
    hbm = pl.BlockSpec(memory_space=pltpu.HBM)
    targets, slots = weights.shape[2:4]
    width = side + 2
    flat = (width * width + 1, levels, cells)
    edges = edge_start(len(WAYS), side)
    hops = len(halo_copies(side))
    pairs = targets * slots // 2
    cost = pl.CostEstimate(
        flops=2 * targets * slots * levels * cells * cells,
        bytes_accessed=weights.size * 2,
        transcendentals=0,
    )
    limit = 50 * 1024 * 1024
    whole, rows, held_counts = (
        pltpu.with_memory_space_constraint(x, pltpu.HBM)
        for x in (weights, jnp.swapaxes(source_ids, 2, 3), counts)
    )
    part, place = pl.pallas_call(
        functools.partial(adjoint_kernel, side, sizes[1]),
        out_shape=[
            jax.ShapeDtypeStruct(flat, jnp.float32),
            jax.ShapeDtypeStruct((slots, targets), jnp.int32),
        ],
        in_specs=[hbm, hbm, hbm, hbm],
        out_specs=[vmem, vmem],
        scratch_shapes=[
            pltpu.VMEM(cotangent.shape[2:], cotangent.dtype),
            pltpu.VMEM((targets * slots, cells, weights.shape[5]), weights.dtype),
            pltpu.VMEM((slots, targets), jnp.int32),
            pltpu.VMEM((1, targets), jnp.int32),
            pltpu.SMEM((1, targets), jnp.int32),
            pltpu.SMEM((slots, targets), jnp.int32),
            pltpu.SMEM((pairs + CHUNK + slots,), jnp.int32),
            pltpu.SMEM((pairs + CHUNK + slots,), jnp.int32),
            pltpu.SemaphoreType.DMA((targets,)),
            pltpu.SemaphoreType.DMA((5,)),
        ],
        compiler_params=pltpu.CompilerParams(vmem_limit_bytes=limit),
        cost_estimate=cost,
        name="adjoint",
    )(rows, held_counts, pltpu.with_memory_space_constraint(cotangent, pltpu.HBM), whole)
    ways = len(WAYS)
    coded = [
        pltpu.VMEM((edges, levels, cells), jnp.int16),
        pltpu.VMEM((edges, 1, cells), jnp.float32),
    ]
    results = [
        jax.ShapeDtypeStruct(cotangent.shape, jnp.bfloat16),
        jax.ShapeDtypeStruct(increment.shape, jnp.bfloat16),
    ]
    ocean, adjoint = pl.pallas_call(
        functools.partial(exchange_kernel, sizes),
        out_shape=results,
        in_specs=[vmem, vmem, vmem, hbm],
        out_specs=[vmem, vmem],
        scratch_shapes=coded + coded + [
            pltpu.VMEM((2, levels, cells), jnp.float32),
            pltpu.VMEM(increment.shape, jnp.float32),
            pltpu.VMEM(flat, increment.dtype),
            pltpu.SMEM((slots, targets), jnp.int32),
            pltpu.VMEM(weights.shape[2:], weights.dtype),
            pltpu.SemaphoreType.DMA((targets,)),
            pltpu.SemaphoreType.DMA((1,)),
        ] + [pltpu.SemaphoreType.DMA((hops,))] * 2 + [pltpu.SemaphoreType.DMA((ways,))] * 4
        + [pltpu.SemaphoreType.DMA((2,))] * 4,
        compiler_params=pltpu.CompilerParams(
            collective_id=0, has_side_effects=True, vmem_limit_bytes=limit
        ),
        cost_estimate=cost,
        name="exchange",
    )(place, increment, part, whole)
    return pl.pallas_call(
        deliver_kernel,
        out_shape=results,
        in_specs=[vmem] * 2,
        out_specs=[hbm] * 2,
        scratch_shapes=[pltpu.SemaphoreType.DMA((SHARES + 1,))],
        compiler_params=pltpu.CompilerParams(vmem_limit_bytes=limit),
        name="deliver",
    )(ocean, adjoint)


def solution(mesh):
    placed = (
        P("lat", "lon", None, None),
        P("lat", "lon", None, None, None),
        P("lat", "lon", None, None, None, None),
        P("lat", "lon", None, None),
        P("lat", "lon", None),
    )
    return jax.shard_map(
        body,
        mesh=mesh,
        in_specs=placed,
        out_specs=(P("lat", "lon", None, None, None), P("lat", "lon", None, None)),
        check_vma=False,
    )
```
